32 devices in a mesh: dp: 2 (over x), tp: 16 (over z, y, core).
Axes of the slice: x: 2, y: 2, z: 4, core: 2. Of those that a mesh axis runs over, the one named last changes fastest.
Arguments:
- hidden: bfloat16 [512, 2304], P('dp', 'tp'), parts along dimension 0
- cand_ids: int32 [512, 4], P('dp'), parts along dimension 0
- norm_scale: bfloat16 [2304], P('tp')
- emb_table: bfloat16 [256000, 2304], P('tp')
Outputs:
- output 1: float32 [512], P('dp'), parts along dimension 0
- output 2: float32 [512, 4], P('dp'), parts along dimension 0
- output 3: bfloat16 [512, 256000], P('dp', 'tp'), parts along dimension 0
There are 2 independent parts. The reference program is written for one: setup_inputs(seed, part) draws one part's arguments, and reference() takes and returns one part's arrays. A program takes and returns all parts, laid end to end along the dimension named above; an argument that names none is the same for every part.
All inputs are finite; a program needn't handle non-finite values.
Results may differ from the reference program's by a relative error of at most 0.001.
Values are sent between devices in bfloat16 or wider.
A program may use at most 1 GiB of HBM per device.

```python
import jax
import jax.numpy as jnp
from jax import lax

BATCH = 256
D = 2304
V = 256000
CANDIDATES = 4
TABLE_BLOCKS = 64
NORM_EPS = 1e-6
SOFT_CAP = 30.0


def draw_table(key):
    block_keys = jax.random.split(key, TABLE_BLOCKS)

    def one_block(blk_key):
        block_vals = jax.random.normal(blk_key, (V // TABLE_BLOCKS, D), jnp.float32)
        return (block_vals * (10.0 * D ** -0.5)).astype(jnp.bfloat16)

    return lax.map(one_block, block_keys).reshape(V, D)


def setup_inputs(seed: int = 0, part: int = 0) -> dict:
    part_key = jax.random.fold_in(jax.random.key(seed), part)
    key_hidden, key_rows, key_cand = jax.random.split(part_key, 3)
    key_scale, key_table = jax.random.split(jax.random.key(seed + 1))
    col_gain = jnp.exp(jnp.linspace(-1.0, 1.0, D))
    row_gain = jnp.exp(jax.random.uniform(key_rows, (BATCH, 1), jnp.float32, -0.5, 0.5))
    hidden = (jax.random.normal(key_hidden, (BATCH, D), jnp.float32) * col_gain * row_gain).astype(jnp.bfloat16)
    cand_ids = jax.random.randint(key_cand, (BATCH, CANDIDATES), 0, V, jnp.int32)
    cand_ids = cand_ids.at[0, 0].set(0).at[BATCH - 1, CANDIDATES - 1].set(V - 1)
    norm_scale = (0.5 * jax.random.normal(key_scale, (D,), jnp.float32)).astype(jnp.bfloat16)
    emb_table = draw_table(key_table)
    return {"hidden": hidden, "cand_ids": cand_ids, "norm_scale": norm_scale, "emb_table": emb_table}


def reference(hidden, cand_ids, norm_scale, emb_table):
    hidden_f32 = hidden.astype(jnp.float32)
    mean_sq = jnp.mean(hidden_f32 * hidden_f32, axis=1, keepdims=True)
    normed = (hidden_f32 * lax.rsqrt(mean_sq + NORM_EPS) * (1.0 + norm_scale.astype(jnp.float32))).astype(jnp.bfloat16)
    logits = jnp.dot(normed, emb_table.T, preferred_element_type=jnp.float32)
    capped = SOFT_CAP * jnp.tanh(logits / SOFT_CAP)
    row_max = jnp.max(capped, axis=1, keepdims=True)
    row_lse = row_max[:, 0] + jnp.log(jnp.sum(jnp.exp(capped - row_max), axis=1))
    log_probs = capped - row_lse[:, None]
    cand_logp = jnp.take_along_axis(log_probs, cand_ids, axis=1)
    return row_lse, cand_logp, log_probs.astype(jnp.bfloat16)
```

```python
import functools

import jax
import jax.numpy as jnp
from jax import lax
from jax.experimental import pallas as pl
from jax.experimental.pallas import tpu as pltpu
from jax.sharding import PartitionSpec as P

NORM_EPS = 1e-6
SOFT_CAP = 30.0
MESH = pl.DeviceIdType.MESH
CORES, YS = 2, 2

TILE = 1600
SLOTS = 5
PIECE = 160
GROUP = 16
OUT_TILE = 3200


def stream_kernel(
    n_dev, n_feat, hid_ref, scale_ref, ids_ref, table_ref, capped_ref, lse_ref, cand_ref,
    ring, za, zb, rows, scales, normed, ids8, stats,
    ring_sem, own_sem, row_send, row_recv, scale_send, scale_recv, stat_send, stat_recv,
):
    d_loc, batch = hid_ref.shape
    vocab = table_ref.shape[0]
    tile = ring.shape[1]
    n_slots = ring.shape[0]
    n_tiles = vocab // tile
    piece = min(PIECE, tile // 2)
    n_cand = ids_ref.shape[0]

    me = lax.axis_index("tp")
    core = lax.rem(me, CORES)
    y = lax.rem(me // CORES, YS)
    z = me // (CORES * YS)
    n_z = n_dev // (CORES * YS)

    def index(z_, y_, c_):
        return (z_ * YS + y_) * CORES + c_

    def table_copy(b):
        slot = lax.rem(b, n_slots)
        return pltpu.make_async_copy(table_ref.at[pl.ds(b * tile, tile), :], ring.at[slot], ring_sem.at[slot])

    own_copy = pltpu.make_async_copy(hid_ref, rows.at[me], own_sem.at[0])
    own_copy.start()
    own_scale = pltpu.make_async_copy(scale_ref, scales.at[me], own_sem.at[1])
    own_scale.start()
    for b in range(n_slots):
        table_copy(b).start()

    barrier = pltpu.get_barrier_semaphore()
    for step in range(1, n_dev):
        pl.semaphore_signal(barrier, inc=1, device_id={"tp": lax.rem(me + step, n_dev)}, device_id_type=MESH)
    pl.semaphore_wait(barrier, n_dev - 1)

    own_copy.wait()
    own_scale.wait()

    def row_copy(slab, to, sem):
        return pltpu.make_async_remote_copy(
            src_ref=rows.at[slab], dst_ref=rows.at[slab], send_sem=row_send.at[sem], recv_sem=row_recv.at[slab],
            device_id={"tp": to}, device_id_type=MESH)

    def scale_copy(slab, to, sem):
        return pltpu.make_async_remote_copy(
            src_ref=scales.at[slab], dst_ref=scales.at[slab], send_sem=scale_send.at[sem], recv_sem=scale_recv.at[slab],
            device_id={"tp": to}, device_id_type=MESH)

    sibling = index(z, y, 1 - core)
    across = index(z, 1 - y, core)
    far_z = [z + 1 - 2 * lax.rem(z, 2), z + 2 - 4 * (z // 2), 3 - z] if n_z == 4 else [1 - z]
    sends = []

    def send(slab, to):
        copy = row_copy(slab, to, len(sends))
        copy.start()
        sends.append(copy)

    def arrive(slab):
        row_copy(slab, me, 0).wait_recv()

    send(me, across)
    for z_ in far_z:
        send(me, index(z_, y, core))
    send(me, sibling)
    scale_sends = []
    for step in range(1, n_dev):
        copy = scale_copy(me, lax.rem(me + step, n_dev), step - 1)
        copy.start()
        scale_sends.append(copy)

    for k in range(n_cand):
        ids8[8 * k:8 * k + 8, :] = jnp.broadcast_to(ids_ref[k:k + 1, :] - me * vocab, (8, batch))

    def squares(slab):
        f32 = rows[slab].astype(jnp.float32)
        return jnp.sum(f32 * f32, axis=0, keepdims=True)

    total = squares(me)
    for z_ in [z] + far_z:
        if z_ is not z:
            slab = index(z_, y, core)
            arrive(slab)
            send(slab, across)
            send(slab, sibling)
            total += squares(slab)
        slab = index(z_, 1 - y, core)
        arrive(slab)
        send(slab, sibling)
        total += squares(slab)
        for y_ in (y, 1 - y):
            slab = index(z_, y_, 1 - core)
            arrive(slab)
            total += squares(slab)
    for step in range(1, n_dev):
        scale_copy(lax.rem(me + step, n_dev), me, 0).wait_recv()

    inv = lax.rsqrt(total * (1.0 / n_feat) + NORM_EPS)
    wide = scales.shape[2]
    pad = [scales[d] for d in range(n_dev)] + [jnp.zeros((128 - n_dev, wide), jnp.float32)]
    scale_cols = jnp.concatenate(pad, axis=0).T
    for d in range(n_dev):
        gain = 1.0 + scale_cols[:d_loc, d:d + 1]
        normed[d * d_loc:(d + 1) * d_loc, :] = (rows[d].astype(jnp.float32) * inv * gain).astype(jnp.bfloat16)

    def tile_step(b, slot, dst, src, row0, carry):
        weights = normed[...]
        sums, picks = carry[0], list(carry[1:])
        for h in range(tile // piece):
            if dst is not None:
                dst[h * piece:(h + 1) * piece, :] = jnp.dot(
                    ring[slot, h * piece:(h + 1) * piece, :], weights, preferred_element_type=jnp.float32)
            for g in range(h * piece, (h + 1) * piece, GROUP):
                capped = jnp.tanh(src[g:g + GROUP, :] * (1.0 / SOFT_CAP)) * SOFT_CAP
                capped_ref[pl.ds(pl.multiple_of(row0 + g, 8), GROUP), :] = capped
                expd = jnp.exp(capped)
                for q in range(0, GROUP, 8):
                    sums = sums + expd[q:q + 8]
                    token = lax.broadcasted_iota(jnp.int32, (8, batch), 0) + (row0 + g + q)
                    for k in range(n_cand):
                        picks[k] = jnp.where(token == ids8[8 * k:8 * k + 8, :], capped[q:q + 8], picks[k])
        return (sums, *picks)

    zero = jnp.zeros((8, batch), jnp.float32)

    def pair(i, carry):
        b = 2 * i
        table_copy(b).wait()
        table_copy(b + 1).wait()
        for b_ in (b - 2, b - 1):
            @pl.when((b_ >= 0) & (b_ + n_slots < n_tiles))
            def _():
                table_copy(b_ + n_slots).start()
        first = jnp.where(i == 0, 0.0, 1.0)
        carry = tile_step(b, lax.rem(b, n_slots), za, zb, jnp.maximum(b - 1, 0) * tile, carry)
        carry = tuple(first * c for c in carry)
        return tile_step(b + 1, lax.rem(b + 1, n_slots), zb, za, b * tile, carry)

    zb[...] = jnp.zeros_like(zb)
    carry = lax.fori_loop(0, n_tiles // 2, pair, (zero,) * (1 + n_cand))
    carry = tile_step(None, None, None, zb, (n_tiles - 1) * tile, carry)

    mine = [jnp.sum(c, axis=0, keepdims=True) for c in carry]
    stats[me] = jnp.concatenate(mine + [jnp.zeros((7 - n_cand, batch), jnp.float32)], axis=0)

    def stat_copy(slab, to, sem):
        return pltpu.make_async_remote_copy(
            src_ref=stats.at[slab], dst_ref=stats.at[slab], send_sem=stat_send.at[sem], recv_sem=stat_recv.at[slab],
            device_id={"tp": to}, device_id_type=MESH)

    stat_sends = []
    for step in range(1, n_dev):
        copy = stat_copy(me, lax.rem(me + step, n_dev), step - 1)
        copy.start()
        stat_sends.append(copy)
    for copy in sends + scale_sends:
        copy.wait_send()
    for step in range(1, n_dev):
        stat_copy(lax.rem(me + step, n_dev), me, 0).wait_recv()
    joined = stats[0]
    for d in range(1, n_dev):
        joined += stats[d]
    lse = jnp.log(joined[0:1, :])
    lse_ref[...] = lse
    cand_ref[...] = joined[1:1 + n_cand, :] - lse
    for copy in stat_sends:
        copy.wait_send()


def finish_kernel(capped_ref, lse_in, cand_in, out_ref, lse_ref, cand_ref, held, sem):
    tokens = held.shape[2]
    copies = []
    for i in range(held.shape[0]):
        part = (capped_ref[i * tokens:(i + 1) * tokens, :] - lse_in[...]).astype(jnp.bfloat16)
        held[i] = part.T
        copy = pltpu.make_async_copy(held.at[i], out_ref.at[:, pl.ds(i * tokens, tokens)], sem.at[i])
        copy.start()
        copies.append(copy)
    lse_ref[...] = lse_in[...]
    cand_ref[...] = cand_in[...]
    for copy in copies:
        copy.wait()


def solution(mesh):
    n_dev = mesh.shape["tp"]

    def device_step(hidden_blk, cand_ids, scale_blk, table_blk):
        batch, d_loc = hidden_blk.shape
        vocab, n_feat = table_blk.shape
        n_cand = cand_ids.shape[1]
        tile = min(TILE, vocab // 2)
        wide = -(-d_loc // 128) * 128
        scale_row = jnp.pad(scale_blk.astype(jnp.float32)[None, :], ((0, 0), (0, wide - d_loc)))
        any_spec = pl.BlockSpec(memory_space=pl.ANY)
        vmem_spec = pl.BlockSpec(memory_space=pltpu.VMEM)
        dma = pltpu.SemaphoreType.DMA
        capped, lse, cand = pl.pallas_call(
            functools.partial(stream_kernel, n_dev, n_feat),
            out_shape=[
                pltpu.VMEM((vocab, batch), jnp.float32),
                pltpu.VMEM((1, batch), jnp.float32),
                pltpu.VMEM((n_cand, batch), jnp.float32),
            ],
            in_specs=[any_spec, any_spec, vmem_spec, any_spec],
            out_specs=[vmem_spec, vmem_spec, vmem_spec],
            scratch_shapes=[
                pltpu.VMEM((min(SLOTS, vocab // tile), tile, n_feat), jnp.bfloat16),
                pltpu.VMEM((tile, batch), jnp.float32),
                pltpu.VMEM((tile, batch), jnp.float32),
                pltpu.VMEM((n_dev, d_loc, batch), jnp.bfloat16),
                pltpu.VMEM((n_dev, 1, wide), jnp.float32),
                pltpu.VMEM((n_feat, batch), jnp.bfloat16),
                pltpu.VMEM((8 * n_cand, batch), jnp.int32),
                pltpu.VMEM((n_dev, 8, batch), jnp.float32),
                dma((min(SLOTS, vocab // tile),)),
                dma((2,)),
                dma((n_dev,)),
                dma((n_dev,)),
                dma((n_dev,)),
                dma((n_dev,)),
                dma((n_dev,)),
                dma((n_dev,)),
            ],
            compiler_params=pltpu.CompilerParams(
                collective_id=0, has_side_effects=True, vmem_limit_bytes=46 * 1024 * 1024),
            cost_estimate=pl.CostEstimate(
                flops=2 * batch * vocab * n_feat, bytes_accessed=2 * vocab * n_feat, transcendentals=2 * batch * vocab),
            name="stream",
        )(hidden_blk.T, scale_row, cand_ids.T, table_blk)
        out_tile = min(OUT_TILE, vocab // 2)
        log_probs, lse, cand = pl.pallas_call(
            finish_kernel,
            out_shape=[
                jax.ShapeDtypeStruct((batch, vocab), jnp.bfloat16),
                jax.ShapeDtypeStruct((1, batch), jnp.float32),
                jax.ShapeDtypeStruct((n_cand, batch), jnp.float32),
            ],
            in_specs=[vmem_spec, vmem_spec, vmem_spec],
            out_specs=[any_spec, vmem_spec, vmem_spec],
            scratch_shapes=[
                pltpu.VMEM((vocab // out_tile, batch, out_tile), jnp.bfloat16),
                dma((vocab // out_tile,)),
            ],
            compiler_params=pltpu.CompilerParams(vmem_limit_bytes=24 * 1024 * 1024),
            name="finish",
        )(capped, lse, cand)
        return lse.reshape(batch), cand.T, log_probs

    return jax.shard_map(
        device_step,
        mesh=mesh,
        in_specs=(P("dp", "tp"), P("dp", None), P("tp"), P("tp", None)),
        out_specs=(P("dp"), P("dp", None), P("dp", "tp")),
        check_vma=False,
    )
```

```python
import functools

import jax
import jax.numpy as jnp
from jax import lax
from jax.experimental import pallas as pl
from jax.experimental.pallas import tpu as pltpu
from jax.sharding import PartitionSpec as P

NORM_EPS = 1e-6
SOFT_CAP = 30.0
MESH = pl.DeviceIdType.MESH
CORES, YS = 2, 2

TILE = 1600
SLOTS = 5
PIECE = 160
GROUP = 16
OUT_UNIT = 640
PARTS = 3


def stream_kernel(
    n_dev, n_feat, hid_ref, scale_ref, ids_ref, table_ref, capped_ref, lse_ref, cand_ref,
    ring, za, zb, rows, scales, normed, ids8, stats,
    ring_sem, own_sem, row_send, row_recv, scale_send, scale_recv, stat_send, stat_recv,
):
    d_loc, batch = hid_ref.shape
    vocab = table_ref.shape[0]
    n_slots, tile, _ = ring.shape
    n_tiles = vocab // tile
    piece = min(PIECE, tile // 2)
    n_cand = ids_ref.shape[0]
    parts = row_recv.shape[1]
    part = d_loc // parts

    me = lax.axis_index("tp")
    core = lax.rem(me, CORES)
    y = lax.rem(me // CORES, YS)
    z = me // (CORES * YS)

    def index(z_, y_, c_):
        return (z_ * YS + y_) * CORES + c_

    def table_copy(b):
        slot = lax.rem(b, n_slots)
        return pltpu.make_async_copy(table_ref.at[pl.ds(b * tile, tile), :], ring.at[slot], ring_sem.at[slot])

    own_copy = pltpu.make_async_copy(hid_ref, rows.at[me], own_sem.at[0])
    own_copy.start()
    for b in range(n_slots):
        table_copy(b).start()

    barrier = pltpu.get_barrier_semaphore()
    for step in range(1, n_dev):
        pl.semaphore_signal(barrier, inc=1, device_id={"tp": lax.rem(me + step, n_dev)}, device_id_type=MESH)

    wide = scales.shape[2]
    scale_row = scale_ref[...].astype(jnp.float32)
    scales[me] = jnp.concatenate([scale_row, jnp.zeros((1, wide - d_loc), jnp.float32)], axis=1)
    for k in range(n_cand):
        ids8[8 * k:8 * k + 8, :] = jnp.broadcast_to(ids_ref[k:k + 1, :] - me * vocab, (8, batch))

    own_copy.wait()
    pl.semaphore_wait(barrier, n_dev - 1)

    sends = []

    def row_copy(slab, p, to, sem):
        where = rows.at[slab, p * part:(p + 1) * part, :]
        return pltpu.make_async_remote_copy(
            src_ref=where, dst_ref=where, send_sem=row_send.at[sem, p], recv_sem=row_recv.at[slab, p],
            device_id={"tp": to}, device_id_type=MESH)

    def send(k, slab, p, to):
        copy = row_copy(slab, p, to, k)
        copy.start()
        sends.append(copy)

    def arrive(slab, p):
        row_copy(slab, p, me, 0).wait_recv()

    def scale_copy(slab, to, sem):
        return pltpu.make_async_remote_copy(
            src_ref=scales.at[slab], dst_ref=scales.at[slab], send_sem=scale_send.at[sem], recv_sem=scale_recv.at[slab],
            device_id={"tp": to}, device_id_type=MESH)

    def squares(slab):
        f32 = rows[slab].astype(jnp.float32)
        return jnp.sum(f32 * f32, axis=0, keepdims=True)

    sibling = index(z, y, 1 - core)
    across = index(z, 1 - y, core)
    far_z = [z + 1 - 2 * lax.rem(z, 2), z + 2 - 4 * (z // 2), 3 - z]

    for p in range(parts):
        send(0, me, p, across)
        send(1, me, p, sibling)
    for j, z_ in enumerate(far_z):
        for p in range(parts):
            send(2 + j, me, p, index(z_, y, core))
    for step in range(1, n_dev):
        copy = scale_copy(me, lax.rem(me + step, n_dev), step - 1)
        copy.start()
        sends.append(copy)

    total = squares(me)

    def take_across(k, z_):
        slab = index(z_, 1 - y, core)
        for p in range(parts):
            arrive(slab, p)
            send(k, slab, p, sibling)
        return squares(slab)

    def take_column(k, z_):
        slab = index(z_, y, core)
        for p in range(parts):
            arrive(slab, p)
            send(k, slab, p, across)
            send(k + 1, slab, p, sibling)
        return squares(slab)

    total += take_across(5, z)
    total += take_column(6, far_z[0])
    total += take_column(8, far_z[1])
    total += take_across(12, far_z[0])
    total += take_column(10, far_z[2])
    total += take_across(13, far_z[1])
    total += take_across(14, far_z[2])
    for step in range(1, n_dev):
        scale_copy(lax.rem(me + step, n_dev), me, 0).wait_recv()
    pad = [scales[d] for d in range(n_dev)] + [jnp.zeros((128 - n_dev, wide), jnp.float32)]
    scale_cols = jnp.concatenate(pad, axis=0).T
    for z_ in [z] + far_z:
        for y_ in (y, 1 - y):
            slab = index(z_, y_, 1 - core)
            for p in range(parts):
                arrive(slab, p)
            total += squares(slab)

    inv = lax.rsqrt(total * (1.0 / n_feat) + NORM_EPS)
    for d in range(n_dev):
        gain = 1.0 + scale_cols[:d_loc, d:d + 1]
        normed[d * d_loc:(d + 1) * d_loc, :] = (rows[d].astype(jnp.float32) * inv * gain).astype(jnp.bfloat16)

    def dot_piece(b, dst, h):
        at = pl.ds(pl.multiple_of(h * piece, 16), piece)
        dst[at, :] = jnp.dot(ring[lax.rem(b, n_slots), at, :], normed[...], preferred_element_type=jnp.float32)

    def epilogue(src, row0, h, carry):
        def group(g, carry):
            at = h * piece + g * GROUP
            sums, picks = carry[0], list(carry[1:])
            capped = jnp.tanh(src[pl.ds(pl.multiple_of(at, 8), GROUP), :] * (1.0 / SOFT_CAP)) * SOFT_CAP
            capped_ref[pl.ds(pl.multiple_of(row0 + at, 8), GROUP), :] = capped
            expd = jnp.exp(capped)
            for q in range(0, GROUP, 8):
                sums = sums + expd[q:q + 8]
                token = lax.broadcasted_iota(jnp.int32, (8, batch), 0) + (row0 + at + q)
                for k in range(n_cand):
                    picks[k] = jnp.where(token == ids8[8 * k:8 * k + 8, :], capped[q:q + 8], picks[k])
            return (sums, *picks)

        return lax.fori_loop(0, piece // GROUP, group, carry, unroll=True)

    def step(b, dst, src, carry):
        table_copy(b).wait()

        def body(h, carry):
            dot_piece(b, dst, h)
            return carry if src is None else epilogue(src, (b - 1) * tile, h, carry)

        carry = lax.fori_loop(0, tile // piece, body, carry, unroll=True)
        @pl.when(b + n_slots < n_tiles)
        def _():
            table_copy(b + n_slots).start()
        return carry

    carry = (jnp.zeros((8, batch), jnp.float32),) * (1 + n_cand)
    carry = step(0, za, None, carry)

    def pair(i, carry):
        carry = step(2 * i + 1, zb, za, carry)
        return step(2 * i + 2, za, zb, carry)

    carry = lax.fori_loop(0, n_tiles // 2 - 1, pair, carry)
    last = n_tiles - 1
    carry = step(last, zb, za, carry)
    carry = lax.fori_loop(0, tile // piece, lambda h, c: epilogue(zb, last * tile, h, c), carry, unroll=True)

    mine = [jnp.sum(c, axis=0, keepdims=True) for c in carry]
    stats[me] = jnp.concatenate(mine + [jnp.zeros((7 - n_cand, batch), jnp.float32)], axis=0)

    def stat_copy(slab, to, sem):
        return pltpu.make_async_remote_copy(
            src_ref=stats.at[slab], dst_ref=stats.at[slab], send_sem=stat_send.at[sem], recv_sem=stat_recv.at[slab],
            device_id={"tp": to}, device_id_type=MESH)

    stat_sends = []
    for step_ in range(1, n_dev):
        copy = stat_copy(me, lax.rem(me + step_, n_dev), step_ - 1)
        copy.start()
        stat_sends.append(copy)
    for copy in sends:
        copy.wait_send()
    for step_ in range(1, n_dev):
        d = lax.rem(me + step_, n_dev)
        stat_copy(d, me, 0).wait_recv()
    joined = stats[0]
    for d in range(1, n_dev):
        joined += stats[d]
    lse = jnp.log(joined[0:1, :])
    lse_ref[...] = lse
    cand_ref[...] = joined[1:1 + n_cand, :] - lse
    for copy in stat_sends:
        copy.wait_send()


def finish_kernel(capped_ref, lse_in, cand_in, out_ref, lse_ref, cand_ref, held, sem):
    small = [pltpu.make_async_copy(lse_in, lse_ref, sem.at[0]), pltpu.make_async_copy(cand_in, cand_ref, sem.at[1])]
    for copy in small:
        copy.start()
    copies = []
    start = 0
    for i, tokens in enumerate(pieces_of(held.shape[1])):
        part = (capped_ref[start:start + tokens, :] - lse_in[...]).astype(jnp.bfloat16)
        held[:, start:start + tokens] = part.T
        copy = pltpu.make_async_copy(
            held.at[:, pl.ds(start, tokens)], out_ref.at[:, pl.ds(start, tokens)], sem.at[2 + i])
        copy.start()
        copies.append(copy)
        start += tokens
    for copy in small + copies:
        copy.wait()


def pieces_of(tokens):
    left, out = tokens // OUT_UNIT, []
    for n in (1, 2, 4):
        if left > n + 7:
            out.append(n)
            left -= n
    while left > 6:
        out.append(4)
        left -= 4
    out += {0: [], 1: [1], 2: [1, 1], 3: [2, 1], 4: [3, 1], 5: [3, 1, 1], 6: [3, 2, 1]}[left]
    return [n * OUT_UNIT for n in out]


def solution(mesh):
    n_dev = mesh.shape["tp"]

    def device_step(hidden_blk, cand_ids, scale_blk, table_blk):
        batch, d_loc = hidden_blk.shape
        vocab, n_feat = table_blk.shape
        n_cand = cand_ids.shape[1]
        tile = min(TILE, vocab // 2)
        wide = -(-d_loc // 128) * 128
        parts = PARTS if d_loc % (16 * PARTS) == 0 else 1
        any_spec = pl.BlockSpec(memory_space=pl.ANY)
        vmem_spec = pl.BlockSpec(memory_space=pltpu.VMEM)
        dma = pltpu.SemaphoreType.DMA
        capped, lse, cand = pl.pallas_call(
            functools.partial(stream_kernel, n_dev, n_feat),
            out_shape=[
                pltpu.VMEM((vocab, batch), jnp.float32),
                pltpu.VMEM((1, batch), jnp.float32),
                pltpu.VMEM((n_cand, batch), jnp.float32),
            ],
            in_specs=[any_spec, vmem_spec, vmem_spec, any_spec],
            out_specs=[vmem_spec, vmem_spec, vmem_spec],
            scratch_shapes=[
                pltpu.VMEM((min(SLOTS, vocab // tile), tile, n_feat), jnp.bfloat16),
                pltpu.VMEM((tile, batch), jnp.float32),
                pltpu.VMEM((tile, batch), jnp.float32),
                pltpu.VMEM((n_dev, d_loc, batch), jnp.bfloat16),
                pltpu.VMEM((n_dev, 1, wide), jnp.float32),
                pltpu.VMEM((n_feat, batch), jnp.bfloat16),
                pltpu.VMEM((8 * n_cand, batch), jnp.int32),
                pltpu.VMEM((n_dev, 8, batch), jnp.float32),
                dma((min(SLOTS, vocab // tile),)),
                dma((1,)),
                dma((n_dev, parts)),
                dma((n_dev, parts)),
                dma((n_dev,)),
                dma((n_dev,)),
                dma((n_dev,)),
                dma((n_dev,)),
            ],
            compiler_params=pltpu.CompilerParams(
                collective_id=0, has_side_effects=True, vmem_limit_bytes=46 * 1024 * 1024),
            cost_estimate=pl.CostEstimate(
                flops=2 * batch * vocab * n_feat, bytes_accessed=2 * vocab * n_feat, transcendentals=2 * batch * vocab),
            name="stream",
        )(hidden_blk.T, scale_blk[None, :], cand_ids.T, table_blk)
        log_probs, lse, cand = pl.pallas_call(
            finish_kernel,
            out_shape=[
                jax.ShapeDtypeStruct((batch, vocab), jnp.bfloat16),
                jax.ShapeDtypeStruct((1, batch), jnp.float32),
                jax.ShapeDtypeStruct((n_cand, batch), jnp.float32),
            ],
            in_specs=[vmem_spec, vmem_spec, vmem_spec],
            out_specs=[any_spec, any_spec, any_spec],
            scratch_shapes=[
                pltpu.VMEM((batch, vocab), jnp.bfloat16),
                dma((2 + len(pieces_of(vocab)),)),
            ],
            compiler_params=pltpu.CompilerParams(vmem_limit_bytes=24 * 1024 * 1024),
            name="finish",
        )(capped, lse, cand)
        return lse.reshape(batch), cand.T, log_probs

    return jax.shard_map(
        device_step,
        mesh=mesh,
        in_specs=(P("dp", "tp"), P("dp", None), P("tp"), P("tp", None)),
        out_specs=(P("dp"), P("dp", None), P("dp", "tp")),
        check_vma=False,
    )
```

```python
import functools

import jax
import jax.numpy as jnp
from jax import lax
from jax.experimental import pallas as pl
from jax.experimental.pallas import tpu as pltpu
from jax.sharding import PartitionSpec as P

NORM_EPS = 1e-6
SOFT_CAP = 30.0
MESH = pl.DeviceIdType.MESH
CORES, YS = 2, 2

TILE = 1600
SLOTS = 5
PIECE = 160
GROUP = 16
OUT_UNIT = 640
EARLY = 1
PARTS = 3


def stream_kernel(
    n_dev, n_feat, hid_ref, scale_ref, ids_ref, table_ref, capped_ref, lse_ref, cand_ref,
    ring, za, zb, rows, scales, normed, ids8, stats,
    ring_sem, own_sem, row_send, row_recv, scale_send, scale_recv, stat_send, stat_recv,
):
    d_loc, batch = hid_ref.shape
    vocab = table_ref.shape[0]
    n_slots, tile, _ = ring.shape
    n_tiles = vocab // tile
    piece = min(PIECE, tile // 2)
    n_cand = ids_ref.shape[0]
    parts = row_recv.shape[1]
    part = d_loc // parts

    me = lax.axis_index("tp")
    core = lax.rem(me, CORES)
    y = lax.rem(me // CORES, YS)
    z = me // (CORES * YS)

    def index(z_, y_, c_):
        return (z_ * YS + y_) * CORES + c_

    def table_copy(b):
        slot = lax.rem(b, n_slots)
        return pltpu.make_async_copy(table_ref.at[pl.ds(b * tile, tile), :], ring.at[slot], ring_sem.at[slot])

    own_copy = pltpu.make_async_copy(hid_ref, rows.at[me], own_sem.at[0])
    own_copy.start()
    for b in range(EARLY):
        table_copy(b).start()

    barrier = pltpu.get_barrier_semaphore()
    for step in range(1, n_dev):
        pl.semaphore_signal(barrier, inc=1, device_id={"tp": lax.rem(me + step, n_dev)}, device_id_type=MESH)

    wide = scales.shape[2]
    scale_row = scale_ref[...].astype(jnp.float32).reshape(1, d_loc)
    scales[me] = jnp.concatenate([scale_row, jnp.zeros((1, wide - d_loc), jnp.float32)], axis=1)
    for k in range(n_cand):
        ids8[8 * k:8 * k + 8, :] = jnp.broadcast_to(ids_ref[k:k + 1, :] - me * vocab, (8, batch))

    own_copy.wait()
    pl.semaphore_wait(barrier, n_dev - 1)

    sends = []

    def row_copy(slab, p, to, sem):
        where = rows.at[slab, p * part:(p + 1) * part, :]
        return pltpu.make_async_remote_copy(
            src_ref=where, dst_ref=where, send_sem=row_send.at[sem, p], recv_sem=row_recv.at[slab, p],
            device_id={"tp": to}, device_id_type=MESH)

    def send(k, slab, p, to):
        copy = row_copy(slab, p, to, k)
        copy.start()
        sends.append(copy)

    def arrive(slab, p):
        row_copy(slab, p, me, 0).wait_recv()

    def scale_copy(slab, to, sem):
        return pltpu.make_async_remote_copy(
            src_ref=scales.at[slab], dst_ref=scales.at[slab], send_sem=scale_send.at[sem], recv_sem=scale_recv.at[slab],
            device_id={"tp": to}, device_id_type=MESH)

    def squares(slab):
        f32 = rows[slab].astype(jnp.float32)
        return jnp.sum(f32 * f32, axis=0, keepdims=True)

    sibling = index(z, y, 1 - core)
    across = index(z, 1 - y, core)
    far_z = [z + 1 - 2 * lax.rem(z, 2), z + 2 - 4 * (z // 2), 3 - z]

    for p in range(parts):
        send(0, me, p, across)
        send(1, me, p, sibling)
    for j, z_ in enumerate(far_z):
        for p in range(parts):
            send(2 + j, me, p, index(z_, y, core))
    for step in range(1, n_dev):
        copy = scale_copy(me, lax.rem(me + step, n_dev), step - 1)
        copy.start()
        sends.append(copy)

    total = squares(me)

    def take_across(k, z_):
        slab = index(z_, 1 - y, core)
        for p in range(parts):
            arrive(slab, p)
            send(k, slab, p, sibling)
        return squares(slab)

    def take_column(k, z_):
        slab = index(z_, y, core)
        for p in range(parts):
            arrive(slab, p)
            send(k, slab, p, across)
            send(k + 1, slab, p, sibling)
        return squares(slab)

    total += take_across(5, z)
    total += take_column(6, far_z[0])
    total += take_column(8, far_z[1])
    total += take_across(12, far_z[0])
    total += take_column(10, far_z[2])
    total += take_across(13, far_z[1])
    total += take_across(14, far_z[2])
    for b in range(EARLY, n_slots):
        table_copy(b).start()
    for step in range(1, n_dev):
        scale_copy(lax.rem(me + step, n_dev), me, 0).wait_recv()
    pad = [scales[d] for d in range(n_dev)] + [jnp.zeros((128 - n_dev, wide), jnp.float32)]
    scale_cols = jnp.concatenate(pad, axis=0).T
    for z_ in [z] + far_z:
        for y_ in (y, 1 - y):
            slab = index(z_, y_, 1 - core)
            for p in range(parts):
                arrive(slab, p)
            total += squares(slab)

    inv = lax.rsqrt(total * (1.0 / n_feat) + NORM_EPS)
    for d in range(n_dev):
        gain = 1.0 + scale_cols[:d_loc, d:d + 1]
        normed[d * d_loc:(d + 1) * d_loc, :] = (rows[d].astype(jnp.float32) * inv * gain).astype(jnp.bfloat16)

    def dot_piece(b, dst, h):
        at = pl.ds(pl.multiple_of(h * piece, 16), piece)
        dst[at, :] = jnp.dot(ring[lax.rem(b, n_slots), at, :], normed[...], preferred_element_type=jnp.float32)

    def epilogue(src, row0, h, carry):
        def group(g, carry):
            at = h * piece + g * GROUP
            sums, picks = carry[0], list(carry[1:])
            capped = jnp.tanh(src[pl.ds(pl.multiple_of(at, 8), GROUP), :] * (1.0 / SOFT_CAP)) * SOFT_CAP
            capped_ref[pl.ds(pl.multiple_of(row0 + at, 8), GROUP), :] = capped
            expd = jnp.exp(capped)
            for q in range(0, GROUP, 8):
                sums = sums + expd[q:q + 8]
                token = lax.broadcasted_iota(jnp.int32, (8, batch), 0) + (row0 + at + q)
                for k in range(n_cand):
                    picks[k] = jnp.where(token == ids8[8 * k:8 * k + 8, :], capped[q:q + 8], picks[k])
            return (sums, *picks)

        return lax.fori_loop(0, piece // GROUP, group, carry, unroll=True)

    def step(b, dst, src, carry):
        table_copy(b).wait()

        def body(h, carry):
            dot_piece(b, dst, h)
            return carry if src is None else epilogue(src, (b - 1) * tile, h, carry)

        carry = lax.fori_loop(0, tile // piece, body, carry, unroll=True)
        @pl.when(b + n_slots < n_tiles)
        def _():
            table_copy(b + n_slots).start()
        return carry

    carry = (jnp.zeros((8, batch), jnp.float32),) * (1 + n_cand)
    carry = step(0, za, None, carry)

    def pair(i, carry):
        carry = step(2 * i + 1, zb, za, carry)
        return step(2 * i + 2, za, zb, carry)

    carry = lax.fori_loop(0, n_tiles // 2 - 1, pair, carry)
    last = n_tiles - 1
    carry = step(last, zb, za, carry)
    carry = lax.fori_loop(0, tile // piece, lambda h, c: epilogue(zb, last * tile, h, c), carry, unroll=True)

    mine = [jnp.sum(c, axis=0, keepdims=True) for c in carry]
    stats[me] = jnp.concatenate(mine + [jnp.zeros((7 - n_cand, batch), jnp.float32)], axis=0)

    def stat_copy(slab, to, sem):
        return pltpu.make_async_remote_copy(
            src_ref=stats.at[slab], dst_ref=stats.at[slab], send_sem=stat_send.at[sem], recv_sem=stat_recv.at[slab],
            device_id={"tp": to}, device_id_type=MESH)

    stat_sends = []
    for step_ in range(1, n_dev):
        copy = stat_copy(me, lax.rem(me + step_, n_dev), step_ - 1)
        copy.start()
        stat_sends.append(copy)
    for copy in sends:
        copy.wait_send()
    for step_ in range(1, n_dev):
        d = lax.rem(me + step_, n_dev)
        stat_copy(d, me, 0).wait_recv()
    joined = stats[0]
    for d in range(1, n_dev):
        joined += stats[d]
    lse = jnp.log(joined[0:1, :])
    lse_ref[...] = lse
    cand_ref[...] = joined[1:1 + n_cand, :] - lse
    for copy in stat_sends:
        copy.wait_send()


def finish_kernel(capped_ref, lse_in, cand_in, out_ref, lse_ref, cand_ref, held, sem):
    small = [pltpu.make_async_copy(lse_in, lse_ref, sem.at[0]), pltpu.make_async_copy(cand_in, cand_ref, sem.at[1])]
    for copy in small:
        copy.start()
    copies = []
    start = 0
    for i, tokens in enumerate(pieces_of(held.shape[1])):
        part = (capped_ref[start:start + tokens, :] - lse_in[...]).astype(jnp.bfloat16)
        held[:, start:start + tokens] = part.T
        copy = pltpu.make_async_copy(
            held.at[:, pl.ds(start, tokens)], out_ref.at[:, pl.ds(start, tokens)], sem.at[2 + i])
        copy.start()
        copies.append(copy)
        start += tokens
    for copy in small + copies:
        copy.wait()


def pieces_of(tokens):
    left, out = tokens // OUT_UNIT, []
    for n in (1, 2, 4):
        if left > n + 7:
            out.append(n)
            left -= n
    while left > 6:
        out.append(4)
        left -= 4
    out += {0: [], 1: [1], 2: [1, 1], 3: [2, 1], 4: [3, 1], 5: [3, 1, 1], 6: [3, 2, 1]}[left]
    return [n * OUT_UNIT for n in out]


def solution(mesh):
    n_dev = mesh.shape["tp"]

    def device_step(hidden_blk, cand_ids, scale_blk, table_blk):
        batch, d_loc = hidden_blk.shape
        vocab, n_feat = table_blk.shape
        n_cand = cand_ids.shape[1]
        tile = min(TILE, vocab // 2)
        wide = -(-d_loc // 128) * 128
        parts = PARTS if d_loc % (16 * PARTS) == 0 else 1
        any_spec = pl.BlockSpec(memory_space=pl.ANY)
        vmem_spec = pl.BlockSpec(memory_space=pltpu.VMEM)
        dma = pltpu.SemaphoreType.DMA
        capped, lse, cand = pl.pallas_call(
            functools.partial(stream_kernel, n_dev, n_feat),
            out_shape=[
                pltpu.VMEM((vocab, batch), jnp.float32),
                pltpu.VMEM((1, batch), jnp.float32),
                pltpu.VMEM((n_cand, batch), jnp.float32),
            ],
            in_specs=[any_spec, vmem_spec, vmem_spec, any_spec],
            out_specs=[vmem_spec, vmem_spec, vmem_spec],
            scratch_shapes=[
                pltpu.VMEM((min(SLOTS, vocab // tile), tile, n_feat), jnp.bfloat16),
                pltpu.VMEM((tile, batch), jnp.float32),
                pltpu.VMEM((tile, batch), jnp.float32),
                pltpu.VMEM((n_dev, d_loc, batch), jnp.bfloat16),
                pltpu.VMEM((n_dev, 1, wide), jnp.float32),
                pltpu.VMEM((n_feat, batch), jnp.bfloat16),
                pltpu.VMEM((8 * n_cand, batch), jnp.int32),
                pltpu.VMEM((n_dev, 8, batch), jnp.float32),
                dma((min(SLOTS, vocab // tile),)),
                dma((1,)),
                dma((n_dev, parts)),
                dma((n_dev, parts)),
                dma((n_dev,)),
                dma((n_dev,)),
                dma((n_dev,)),
                dma((n_dev,)),
            ],
            compiler_params=pltpu.CompilerParams(
                collective_id=0, has_side_effects=True, vmem_limit_bytes=46 * 1024 * 1024),
            cost_estimate=pl.CostEstimate(
                flops=2 * batch * vocab * n_feat, bytes_accessed=2 * vocab * n_feat, transcendentals=2 * batch * vocab),
            name="stream",
        )(hidden_blk.T, scale_blk, cand_ids.T, table_blk)
        log_probs, lse, cand = pl.pallas_call(
            finish_kernel,
            out_shape=[
                jax.ShapeDtypeStruct((batch, vocab), jnp.bfloat16),
                jax.ShapeDtypeStruct((1, batch), jnp.float32),
                jax.ShapeDtypeStruct((n_cand, batch), jnp.float32),
            ],
            in_specs=[vmem_spec, vmem_spec, vmem_spec],
            out_specs=[any_spec, any_spec, any_spec],
            scratch_shapes=[
                pltpu.VMEM((batch, vocab), jnp.bfloat16),
                dma((2 + len(pieces_of(vocab)),)),
            ],
            compiler_params=pltpu.CompilerParams(vmem_limit_bytes=24 * 1024 * 1024),
            name="finish",
        )(capped, lse, cand)
        return lse.reshape(batch), cand.T, log_probs

    return jax.shard_map(
        device_step,
        mesh=mesh,
        in_specs=(P("dp", "tp"), P("dp", None), P("tp"), P("tp", None)),
        out_specs=(P("dp"), P("dp", None), P("dp", "tp")),
        check_vma=False,
    )
```

```python
import functools

import jax
import jax.numpy as jnp
from jax import lax
from jax.experimental import pallas as pl
from jax.experimental.pallas import tpu as pltpu
from jax.sharding import PartitionSpec as P

NORM_EPS = 1e-6
SOFT_CAP = 30.0
MESH = pl.DeviceIdType.MESH
CORES, YS = 2, 2

TILE = 1600
SLOTS = 5
PIECE = 160
GROUP = 16
OUT_UNIT = 640
EARLY = 2
PARTS = 3


def stream_kernel(
    n_dev, n_feat, hid_ref, scale_ref, ids_ref, table_ref, capped_ref, lse_ref, cand_ref,
    ring, z0, z1, z2, z3, z4, z5, rows, early, normed, ids_wide, stats,
    near_sem, ring_sem, own_sem, row_send, row_recv, early_send, early_recv, stat_send, stat_recv,
):
    d_loc, batch = hid_ref.shape
    vocab = table_ref.shape[0]
    n_slots, tile, _ = ring.shape
    n_tiles = vocab // tile
    piece = min(PIECE, tile // 2)
    n_cand = ids_ref.shape[0]
    parts = row_recv.shape[1]
    part = d_loc // parts

    me = lax.axis_index("tp")
    core = lax.rem(me, CORES)
    y = lax.rem(me // CORES, YS)
    z = me // (CORES * YS)

    def index(z_, y_, c_):
        return (z_ * YS + y_) * CORES + c_

    near = z // (n_dev // (CORES * YS) // 2)
    near_len = max(128, n_feat // 2 // 256 * 256)
    far_len = n_feat - near_len
    near_at = pl.ds(pl.multiple_of(near * far_len, 128), near_len)
    far_at = pl.ds(pl.multiple_of((1 - near) * near_len, 128), far_len)

    def table_copy(b):
        slot = lax.rem(b, n_slots)
        return pltpu.make_async_copy(table_ref.at[pl.ds(b * tile, tile), :], ring.at[slot], ring_sem.at[slot])

    def near_copy(b):
        return pltpu.make_async_copy(
            table_ref.at[pl.ds(b * tile, tile), near_at], ring.at[b, :, near_at], near_sem.at[b])

    def far_copy(b):
        return pltpu.make_async_copy(
            table_ref.at[pl.ds(b * tile, tile), far_at], ring.at[b, :, far_at], ring_sem.at[b])

    own_copy = pltpu.make_async_copy(hid_ref, rows.at[me], own_sem.at[0])
    own_copy.start()
    for b in range(EARLY):
        near_copy(b).start()

    barrier = pltpu.get_barrier_semaphore()
    for step in range(1, n_dev):
        pl.semaphore_signal(barrier, inc=1, device_id={"tp": lax.rem(me + step, n_dev)}, device_id_type=MESH)

    def squares(slab):
        f32 = rows[slab].astype(jnp.float32)
        return jnp.sum(f32 * f32, axis=0, keepdims=True)

    wide = early.shape[2] - batch
    scale_row = scale_ref[...].astype(jnp.float32).reshape(1, d_loc)
    own_copy.wait()
    early[me] = jnp.concatenate([squares(me), scale_row, jnp.zeros((1, wide - d_loc), jnp.float32)], axis=1)
    for k in range(n_cand):
        ids_wide[GROUP * k:GROUP * (k + 1), :] = jnp.broadcast_to(ids_ref[k:k + 1, :] - me * vocab, (GROUP, batch))

    pl.semaphore_wait(barrier, n_dev - 1)

    sends = []

    def row_copy(slab, p, to, sem):
        where = rows.at[slab, p * part:(p + 1) * part, :]
        return pltpu.make_async_remote_copy(
            src_ref=where, dst_ref=where, send_sem=row_send.at[sem, p], recv_sem=row_recv.at[slab, p],
            device_id={"tp": to}, device_id_type=MESH)

    def send(k, slab, p, to):
        copy = row_copy(slab, p, to, k)
        copy.start()
        sends.append(copy)

    def arrive(slab, p):
        row_copy(slab, p, me, 0).wait_recv()

    def early_copy(slab, to, sem):
        return pltpu.make_async_remote_copy(
            src_ref=early.at[slab], dst_ref=early.at[slab], send_sem=early_send.at[sem], recv_sem=early_recv.at[slab],
            device_id={"tp": to}, device_id_type=MESH)

    sibling = index(z, y, 1 - core)
    across = index(z, 1 - y, core)
    far_z = [z + 1 - 2 * lax.rem(z, 2), z + 2 - 4 * (z // 2), 3 - z]

    for step in range(1, n_dev):
        copy = early_copy(me, lax.rem(me + step, n_dev), step - 1)
        copy.start()
        sends.append(copy)
    for p in range(parts):
        send(0, me, p, across)
        send(1, me, p, sibling)
    for j, z_ in enumerate(far_z):
        for p in range(parts):
            send(2 + j, me, p, index(z_, y, core))

    def take_across(k, z_):
        slab = index(z_, 1 - y, core)
        for p in range(parts):
            arrive(slab, p)
            send(k, slab, p, sibling)

    def take_column(k, z_):
        slab = index(z_, y, core)
        for p in range(parts):
            arrive(slab, p)
            send(k, slab, p, across)
            send(k + 1, slab, p, sibling)

    def take_siblings(z_):
        for y_ in (y, 1 - y):
            for p in range(parts):
                arrive(index(z_, y_, 1 - core), p)

    take_across(5, z)
    take_column(6, far_z[0])
    near_copy(EARLY).start()
    take_column(8, far_z[1])
    take_across(12, far_z[0])
    near_copy(EARLY + 1).start()
    take_column(10, far_z[2])
    for b in range(EARLY + 2, n_slots):
        near_copy(b).start()
    for step in range(1, n_dev):
        early_copy(lax.rem(me + step, n_dev), me, 0).wait_recv()
    total = early[0]
    for d in range(1, n_dev):
        total += early[d]
    total = total[:, :batch]
    inv = lax.rsqrt(total * (1.0 / n_feat) + NORM_EPS)
    half = n_dev // 2
    order = [near * half + d for d in range(half)] + [(1 - near) * half + d for d in range(half)]
    pad = [early[d][:, batch:] for d in order] + [jnp.zeros((128 - n_dev, wide), jnp.float32)]
    gains = 1.0 + jnp.concatenate(pad, axis=0).T
    take_siblings(z)
    take_siblings(far_z[0])

    def normalize(places):
        for i in places:
            d = order[i]
            out = (rows[d].astype(jnp.float32) * inv * gains[:d_loc, i:i + 1]).astype(jnp.bfloat16)
            normed[pl.ds(pl.multiple_of(d * d_loc, 16), d_loc), :] = out

    normalize(range(half))

    def near_step(b, dst):
        near_copy(b).wait()

        def body(h, _):
            at = pl.multiple_of(h * piece, 16)
            dst[pl.ds(at, piece), :] = jnp.dot(
                ring[b, pl.ds(at, piece), near_at], normed[near_at, :], preferred_element_type=jnp.float32)
            return 0

        lax.fori_loop(0, tile // piece, body, 0, unroll=True)

    held = (z0, z1, z2, z3, z4, z5)
    near_step(0, z0)
    take_across(13, far_z[1])
    far_copy(0).start()
    near_step(1, z1)
    take_across(14, far_z[2])
    for b in range(1, n_slots):
        far_copy(b).start()
    for b in range(2, n_slots):
        near_step(b, held[b])
    take_siblings(far_z[1])
    take_siblings(far_z[2])
    normalize(range(half, n_dev))

    def dot_piece(b, dst, h):
        at = pl.ds(pl.multiple_of(h * piece, 16), piece)
        dst[at, :] = jnp.dot(ring[lax.rem(b, n_slots), at, :], normed[...], preferred_element_type=jnp.float32)

    def epilogue(src, row0, h, carry):
        ids = [ids_wide[GROUP * k:GROUP * (k + 1), :] for k in range(n_cand)]

        def group(g, carry):
            at = h * piece + g * GROUP
            sums, picks = carry[0], list(carry[1:])
            capped = jnp.tanh(src[pl.ds(pl.multiple_of(at, 8), GROUP), :] * (1.0 / SOFT_CAP)) * SOFT_CAP
            capped_ref[pl.ds(pl.multiple_of(row0 + at, 8), GROUP), :] = capped
            sums = sums + jnp.exp(capped)
            token = lax.broadcasted_iota(jnp.int32, (GROUP, batch), 0) + (row0 + at)
            picks = [jnp.where(token == i, capped, p) for i, p in zip(ids, picks)]
            return (sums, *picks)

        return lax.fori_loop(0, piece // GROUP, group, carry, unroll=True)

    def far_step(b, dst):
        far_copy(b).wait()

        def body(h, _):
            at = pl.multiple_of(h * piece, 16)
            dst[pl.ds(at, piece), :] += jnp.dot(
                ring[b, pl.ds(at, piece), far_at], normed[far_at, :], preferred_element_type=jnp.float32)
            return 0

        lax.fori_loop(0, tile // piece, body, 0, unroll=True)
        if b + n_slots < n_tiles:
            table_copy(b + n_slots).start()

    def full_step(b, dst, done, carry):
        table_copy(b).wait()

        def body(h, carry):
            dot_piece(b, dst, h)
            for t in done:
                carry = epilogue(place(t), t * tile, h, carry)
            return carry

        carry = lax.fori_loop(0, tile // piece, body, carry, unroll=True)
        if b + n_slots < n_tiles:
            table_copy(b + n_slots).start()
        return carry

    def place(t):
        return held[t % len(held)]

    carry = (jnp.zeros((GROUP, batch), jnp.float32),) * (1 + n_cand)
    for b in range(n_slots):
        far_step(b, place(b))
    finished = 0
    for b in range(n_slots, n_tiles):
        done = list(range(finished, min(finished + 2, b)))
        finished += len(done)
        carry = full_step(b, place(b), done, carry)
    for t in range(finished, n_tiles):
        carry = lax.fori_loop(0, tile // piece, lambda h, c, t=t: epilogue(place(t), t * tile, h, c), carry)

    mine = [jnp.sum(c, axis=0, keepdims=True) for c in carry]
    stats[me] = jnp.concatenate(mine, axis=1)

    def stat_copy(slab, to, sem):
        return pltpu.make_async_remote_copy(
            src_ref=stats.at[slab], dst_ref=stats.at[slab], send_sem=stat_send.at[sem], recv_sem=stat_recv.at[slab],
            device_id={"tp": to}, device_id_type=MESH)

    stat_sends = []
    for step_ in range(1, n_dev):
        copy = stat_copy(me, lax.rem(me + step_, n_dev), step_ - 1)
        copy.start()
        stat_sends.append(copy)
    for copy in sends:
        copy.wait_send()
    for step_ in range(1, n_dev):
        d = lax.rem(me + step_, n_dev)
        stat_copy(d, me, 0).wait_recv()
    joined = stats[0]
    for d in range(1, n_dev):
        joined += stats[d]
    lse = jnp.log(joined[:, :batch])
    lse_ref[...] = lse
    for k in range(n_cand):
        cand_ref[k:k + 1, :] = joined[:, (k + 1) * batch:(k + 2) * batch] - lse
    for copy in stat_sends:
        copy.wait_send()


def finish_kernel(capped_ref, lse_in, cand_in, out_ref, lse_ref, cand_ref, held, sem):
    small = [pltpu.make_async_copy(lse_in, lse_ref, sem.at[0]), pltpu.make_async_copy(cand_in, cand_ref, sem.at[1])]
    for copy in small:
        copy.start()
    copies = []
    start = 0
    for i, tokens in enumerate(pieces_of(held.shape[1])):
        part = (capped_ref[start:start + tokens, :] - lse_in[...]).astype(jnp.bfloat16)
        held[:, start:start + tokens] = part.T
        copy = pltpu.make_async_copy(
            held.at[:, pl.ds(start, tokens)], out_ref.at[:, pl.ds(start, tokens)], sem.at[2 + i])
        copy.start()
        copies.append(copy)
        start += tokens
    for copy in small + copies:
        copy.wait()


def pieces_of(tokens):
    left, out = tokens // OUT_UNIT, []
    for n in (1, 2, 4):
        if left > n + 7:
            out.append(n)
            left -= n
    while left > 6:
        out.append(4)
        left -= 4
    out += {0: [], 1: [1], 2: [1, 1], 3: [2, 1], 4: [3, 1], 5: [3, 1, 1], 6: [3, 2, 1]}[left]
    return [n * OUT_UNIT for n in out]


def solution(mesh):
    n_dev = mesh.shape["tp"]

    def device_step(hidden_blk, cand_ids, scale_blk, table_blk):
        batch, d_loc = hidden_blk.shape
        vocab, n_feat = table_blk.shape
        n_cand = cand_ids.shape[1]
        tile = min(TILE, vocab // 2)
        wide = -(-d_loc // 128) * 128
        parts = PARTS if d_loc % (16 * PARTS) == 0 else 1
        any_spec = pl.BlockSpec(memory_space=pl.ANY)
        vmem_spec = pl.BlockSpec(memory_space=pltpu.VMEM)
        dma = pltpu.SemaphoreType.DMA
        capped, lse, cand = pl.pallas_call(
            functools.partial(stream_kernel, n_dev, n_feat),
            out_shape=[
                pltpu.VMEM((vocab, batch), jnp.float32),
                pltpu.VMEM((1, batch), jnp.float32),
                pltpu.VMEM((n_cand, batch), jnp.float32),
            ],
            in_specs=[any_spec, vmem_spec, vmem_spec, any_spec],
            out_specs=[vmem_spec, vmem_spec, vmem_spec],
            scratch_shapes=[
                pltpu.VMEM((min(SLOTS, vocab // tile), tile, n_feat), jnp.bfloat16),
                *[pltpu.VMEM((tile, batch), jnp.float32)] * 6,
                pltpu.VMEM((n_dev, d_loc, batch), jnp.bfloat16),
                pltpu.VMEM((n_dev, 1, batch + wide), jnp.float32),
                pltpu.VMEM((n_feat, batch), jnp.bfloat16),
                pltpu.VMEM((GROUP * n_cand, batch), jnp.int32),
                pltpu.VMEM((n_dev, 1, (1 + n_cand) * batch), jnp.float32),
                dma((min(SLOTS, vocab // tile),)),
                dma((min(SLOTS, vocab // tile),)),
                dma((1,)),
                dma((n_dev, parts)),
                dma((n_dev, parts)),
                dma((n_dev,)),
                dma((n_dev,)),
                dma((n_dev,)),
                dma((n_dev,)),
            ],
            compiler_params=pltpu.CompilerParams(
                collective_id=0, has_side_effects=True, vmem_limit_bytes=48 * 1024 * 1024),
            cost_estimate=pl.CostEstimate(
                flops=2 * batch * vocab * n_feat, bytes_accessed=2 * vocab * n_feat, transcendentals=2 * batch * vocab),
            name="stream",
        )(hidden_blk.T, scale_blk, cand_ids.T, table_blk)
        log_probs, lse, cand = pl.pallas_call(
            finish_kernel,
            out_shape=[
                jax.ShapeDtypeStruct((batch, vocab), jnp.bfloat16),
                jax.ShapeDtypeStruct((1, batch), jnp.float32),
                jax.ShapeDtypeStruct((n_cand, batch), jnp.float32),
            ],
            in_specs=[vmem_spec, vmem_spec, vmem_spec],
            out_specs=[any_spec, any_spec, any_spec],
            scratch_shapes=[
                pltpu.VMEM((batch, vocab), jnp.bfloat16),
                dma((2 + len(pieces_of(vocab)),)),
            ],
            compiler_params=pltpu.CompilerParams(vmem_limit_bytes=24 * 1024 * 1024),
            name="finish",
        )(capped, lse, cand)
        return lse.reshape(batch), cand.T, log_probs

    return jax.shard_map(
        device_step,
        mesh=mesh,
        in_specs=(P("dp", "tp"), P("dp", None), P("tp"), P("tp", None)),
        out_specs=(P("dp"), P("dp", None), P("dp", "tp")),
        check_vma=False,
    )
```

```python
import functools

import jax
import jax.numpy as jnp
from jax import lax
from jax.experimental import pallas as pl
from jax.experimental.pallas import tpu as pltpu
from jax.sharding import PartitionSpec as P

NORM_EPS = 1e-6
SOFT_CAP = 30.0
MESH = pl.DeviceIdType.MESH
CORES, YS = 2, 2

TILE = 1600
SLOTS = 5
PIECE = 160
GROUP = 16
OUT_UNIT = 640
EARLY = 2
PARTS = 3


def stream_kernel(
    n_dev, n_feat, hid_ref, scale_ref, ids_ref, table_ref, capped_ref, lse_ref, cand_ref,
    ring, z0, z1, z2, z3, z4, z5, rows, early, normed, ids_wide, stats,
    near_sem, ring_sem, own_sem, row_send, row_recv, early_send, early_recv, stat_send, stat_recv,
):
    d_loc, batch = hid_ref.shape
    vocab = table_ref.shape[0]
    n_slots, tile, _ = ring.shape
    n_tiles = vocab // tile
    piece = min(PIECE, tile // 2)
    n_cand = ids_ref.shape[0]
    parts = row_recv.shape[1]
    part = d_loc // parts

    me = lax.axis_index("tp")
    core = lax.rem(me, CORES)
    y = lax.rem(me // CORES, YS)
    z = me // (CORES * YS)

    def index(z_, y_, c_):
        return (z_ * YS + y_) * CORES + c_

    near = z // (n_dev // (CORES * YS) // 2)
    near_len = max(128, n_feat // 2 // 256 * 256)
    far_len = n_feat - near_len
    near_at = pl.ds(pl.multiple_of(near * far_len, 128), near_len)
    far_at = pl.ds(pl.multiple_of((1 - near) * near_len, 128), far_len)

    def table_copy(b):
        slot = lax.rem(b, n_slots)
        return pltpu.make_async_copy(table_ref.at[pl.ds(b * tile, tile), :], ring.at[slot], ring_sem.at[slot])

    def near_copy(b):
        return pltpu.make_async_copy(
            table_ref.at[pl.ds(b * tile, tile), near_at], ring.at[b, :, near_at], near_sem.at[b])

    def far_copy(b):
        return pltpu.make_async_copy(
            table_ref.at[pl.ds(b * tile, tile), far_at], ring.at[b, :, far_at], ring_sem.at[b])

    own_copy = pltpu.make_async_copy(hid_ref, rows.at[me], own_sem.at[0])
    own_copy.start()
    for b in range(EARLY):
        near_copy(b).start()

    barrier = pltpu.get_barrier_semaphore()
    for step in range(1, n_dev):
        pl.semaphore_signal(barrier, inc=1, device_id={"tp": lax.rem(me + step, n_dev)}, device_id_type=MESH)

    def squares(slab):
        f32 = rows[slab].astype(jnp.float32)
        return jnp.sum(f32 * f32, axis=0, keepdims=True)

    wide = early.shape[2] - batch
    scale_row = scale_ref[...].astype(jnp.float32).reshape(1, d_loc)
    own_copy.wait()
    early[me] = jnp.concatenate([squares(me), scale_row, jnp.zeros((1, wide - d_loc), jnp.float32)], axis=1)
    for k in range(n_cand):
        ids_wide[GROUP * k:GROUP * (k + 1), :] = jnp.broadcast_to(ids_ref[k:k + 1, :] - me * vocab, (GROUP, batch))

    pl.semaphore_wait(barrier, n_dev - 1)

    sends = []

    def row_copy(slab, p, to, sem):
        where = rows.at[slab, p * part:(p + 1) * part, :]
        return pltpu.make_async_remote_copy(
            src_ref=where, dst_ref=where, send_sem=row_send.at[sem, p], recv_sem=row_recv.at[slab, p],
            device_id={"tp": to}, device_id_type=MESH)

    def send(k, slab, p, to):
        copy = row_copy(slab, p, to, k)
        copy.start()
        sends.append(copy)

    def arrive(slab, p):
        row_copy(slab, p, me, 0).wait_recv()

    def early_copy(slab, to, sem):
        return pltpu.make_async_remote_copy(
            src_ref=early.at[slab], dst_ref=early.at[slab], send_sem=early_send.at[sem], recv_sem=early_recv.at[slab],
            device_id={"tp": to}, device_id_type=MESH)

    sibling = index(z, y, 1 - core)
    across = index(z, 1 - y, core)
    far_z = [z + 1 - 2 * lax.rem(z, 2), z + 2 - 4 * (z // 2), 3 - z]

    for step in range(1, n_dev):
        copy = early_copy(me, lax.rem(me + step, n_dev), step - 1)
        copy.start()
        sends.append(copy)
    for p in range(parts):
        send(0, me, p, across)
        send(1, me, p, sibling)
    for j, z_ in enumerate(far_z):
        for p in range(parts):
            send(2 + j, me, p, index(z_, y, core))

    def take_across(k, z_):
        slab = index(z_, 1 - y, core)
        for p in range(parts):
            arrive(slab, p)
            send(k, slab, p, sibling)

    def take_column(k, z_):
        slab = index(z_, y, core)
        for p in range(parts):
            arrive(slab, p)
            send(k, slab, p, across)
            send(k + 1, slab, p, sibling)

    def take_siblings(z_):
        for y_ in (y, 1 - y):
            for p in range(parts):
                arrive(index(z_, y_, 1 - core), p)

    take_across(5, z)
    take_column(6, far_z[0])
    near_copy(EARLY).start()
    take_column(8, far_z[1])
    take_across(12, far_z[0])
    near_copy(EARLY + 1).start()
    for step in range(1, n_dev):
        early_copy(lax.rem(me + step, n_dev), me, 0).wait_recv()
    total = early[0]
    for d in range(1, n_dev):
        total += early[d]
    total = total[:, :batch]
    inv = lax.rsqrt(total * (1.0 / n_feat) + NORM_EPS)
    half = n_dev // 2
    order = [near * half + d for d in range(half)] + [(1 - near) * half + d for d in range(half)]
    pad = [early[d][:, batch:] for d in order] + [jnp.zeros((128 - n_dev, wide), jnp.float32)]
    gains = 1.0 + jnp.concatenate(pad, axis=0).T
    take_siblings(z)
    take_siblings(far_z[0])

    def normalize(places):
        for i in places:
            d = order[i]
            out = (rows[d].astype(jnp.float32) * inv * gains[:d_loc, i:i + 1]).astype(jnp.bfloat16)
            normed[pl.ds(pl.multiple_of(d * d_loc, 16), d_loc), :] = out

    normalize(range(half))

    def near_step(b, dst):
        near_copy(b).wait()

        def body(h, _):
            at = pl.multiple_of(h * piece, 16)
            dst[pl.ds(at, piece), :] = jnp.dot(
                ring[b, pl.ds(at, piece), near_at], normed[near_at, :], preferred_element_type=jnp.float32)
            return 0

        lax.fori_loop(0, tile // piece, body, 0, unroll=True)

    held = (z0, z1, z2, z3, z4, z5)
    near_step(0, held[0])
    take_column(10, far_z[2])
    for b in range(EARLY + 2, n_slots):
        near_copy(b).start()
    far_copy(0).start()
    near_step(1, held[1])
    take_across(13, far_z[1])
    far_copy(1).start()
    near_step(2, held[2])
    take_across(14, far_z[2])
    for b in range(2, n_slots):
        far_copy(b).start()
    for b in range(3, n_slots):
        near_step(b, held[b])
    take_siblings(far_z[1])
    take_siblings(far_z[2])
    normalize(range(half, n_dev))

    def dot_piece(b, dst, h):
        at = pl.ds(pl.multiple_of(h * piece, 16), piece)
        dst[at, :] = jnp.dot(ring[lax.rem(b, n_slots), at, :], normed[...], preferred_element_type=jnp.float32)

    def epilogue(src, row0, h, carry):
        ids = [ids_wide[GROUP * k:GROUP * (k + 1), :] for k in range(n_cand)]

        def group(g, carry):
            at = h * piece + g * GROUP
            sums, picks = carry[0], list(carry[1:])
            capped = jnp.tanh(src[pl.ds(pl.multiple_of(at, 8), GROUP), :] * (1.0 / SOFT_CAP)) * SOFT_CAP
            capped_ref[pl.ds(pl.multiple_of(row0 + at, 8), GROUP), :] = capped
            sums = sums + jnp.exp(capped)
            token = lax.broadcasted_iota(jnp.int32, (GROUP, batch), 0) + (row0 + at)
            picks = [jnp.where(token == i, capped, p) for i, p in zip(ids, picks)]
            return (sums, *picks)

        return lax.fori_loop(0, piece // GROUP, group, carry, unroll=True)

    def far_step(b, dst):
        far_copy(b).wait()

        def body(h, _):
            at = pl.multiple_of(h * piece, 16)
            dst[pl.ds(at, piece), :] += jnp.dot(
                ring[b, pl.ds(at, piece), far_at], normed[far_at, :], preferred_element_type=jnp.float32)
            return 0

        lax.fori_loop(0, tile // piece, body, 0, unroll=True)
        if b + n_slots < n_tiles:
            table_copy(b + n_slots).start()

    def full_step(b, dst, done, carry):
        table_copy(b).wait()

        def body(h, carry):
            dot_piece(b, dst, h)
            for t in done:
                carry = epilogue(place(t), t * tile, h, carry)
            return carry

        carry = lax.fori_loop(0, tile // piece, body, carry, unroll=True)
        if b + n_slots < n_tiles:
            table_copy(b + n_slots).start()
        return carry

    def place(t):
        return held[t % len(held)]

    carry = (jnp.zeros((GROUP, batch), jnp.float32),) * (1 + n_cand)
    for b in range(n_slots):
        far_step(b, place(b))
    finished = 0
    for b in range(n_slots, n_tiles):
        done = list(range(finished, min(finished + 2, b)))
        finished += len(done)
        carry = full_step(b, place(b), done, carry)
    for t in range(finished, n_tiles):
        carry = lax.fori_loop(0, tile // piece, lambda h, c, t=t: epilogue(place(t), t * tile, h, c), carry)

    mine = [jnp.sum(c, axis=0, keepdims=True) for c in carry]
    stats[me] = jnp.concatenate(mine, axis=1)

    def stat_copy(slab, to, sem):
        return pltpu.make_async_remote_copy(
            src_ref=stats.at[slab], dst_ref=stats.at[slab], send_sem=stat_send.at[sem], recv_sem=stat_recv.at[slab],
            device_id={"tp": to}, device_id_type=MESH)

    stat_sends = []
    for step_ in range(1, n_dev):
        copy = stat_copy(me, lax.rem(me + step_, n_dev), step_ - 1)
        copy.start()
        stat_sends.append(copy)
    for copy in sends:
        copy.wait_send()
    for step_ in range(1, n_dev):
        d = lax.rem(me + step_, n_dev)
        stat_copy(d, me, 0).wait_recv()
    joined = stats[0]
    for d in range(1, n_dev):
        joined += stats[d]
    lse = jnp.log(joined[:, :batch])
    lse_ref[...] = lse
    for k in range(n_cand):
        cand_ref[k:k + 1, :] = joined[:, (k + 1) * batch:(k + 2) * batch] - lse
    for copy in stat_sends:
        copy.wait_send()


def finish_kernel(capped_ref, lse_in, cand_in, out_ref, lse_ref, cand_ref, held, sem):
    small = [pltpu.make_async_copy(lse_in, lse_ref, sem.at[0]), pltpu.make_async_copy(cand_in, cand_ref, sem.at[1])]
    for copy in small:
        copy.start()
    copies = []
    start = 0
    for i, tokens in enumerate(pieces_of(held.shape[1])):
        part = (capped_ref[start:start + tokens, :] - lse_in[...]).astype(jnp.bfloat16)
        held[:, start:start + tokens] = part.T
        copy = pltpu.make_async_copy(
            held.at[:, pl.ds(start, tokens)], out_ref.at[:, pl.ds(start, tokens)], sem.at[2 + i])
        copy.start()
        copies.append(copy)
        start += tokens
    for copy in small + copies:
        copy.wait()


def pieces_of(tokens):
    left, out = tokens // OUT_UNIT, []
    for n in (1, 2, 4):
        if left > n + 7:
            out.append(n)
            left -= n
    while left > 6:
        out.append(4)
        left -= 4
    out += {0: [], 1: [1], 2: [1, 1], 3: [2, 1], 4: [3, 1], 5: [3, 1, 1], 6: [3, 2, 1]}[left]
    return [n * OUT_UNIT for n in out]


def solution(mesh):
    n_dev = mesh.shape["tp"]

    def device_step(hidden_blk, cand_ids, scale_blk, table_blk):
        batch, d_loc = hidden_blk.shape
        vocab, n_feat = table_blk.shape
        n_cand = cand_ids.shape[1]
        tile = min(TILE, vocab // 2)
        wide = -(-d_loc // 128) * 128
        parts = PARTS if d_loc % (16 * PARTS) == 0 else 1
        any_spec = pl.BlockSpec(memory_space=pl.ANY)
        vmem_spec = pl.BlockSpec(memory_space=pltpu.VMEM)
        dma = pltpu.SemaphoreType.DMA
        capped, lse, cand = pl.pallas_call(
            functools.partial(stream_kernel, n_dev, n_feat),
            out_shape=[
                pltpu.VMEM((vocab, batch), jnp.float32),
                pltpu.VMEM((1, batch), jnp.float32),
                pltpu.VMEM((n_cand, batch), jnp.float32),
            ],
            in_specs=[any_spec, vmem_spec, vmem_spec, any_spec],
            out_specs=[vmem_spec, vmem_spec, vmem_spec],
            scratch_shapes=[
                pltpu.VMEM((min(SLOTS, vocab // tile), tile, n_feat), jnp.bfloat16),
                *[pltpu.VMEM((tile, batch), jnp.float32)] * 6,
                pltpu.VMEM((n_dev, d_loc, batch), jnp.bfloat16),
                pltpu.VMEM((n_dev, 1, batch + wide), jnp.float32),
                pltpu.VMEM((n_feat, batch), jnp.bfloat16),
                pltpu.VMEM((GROUP * n_cand, batch), jnp.int32),
                pltpu.VMEM((n_dev, 1, (1 + n_cand) * batch), jnp.float32),
                dma((min(SLOTS, vocab // tile),)),
                dma((min(SLOTS, vocab // tile),)),
                dma((1,)),
                dma((n_dev, parts)),
                dma((n_dev, parts)),
                dma((n_dev,)),
                dma((n_dev,)),
                dma((n_dev,)),
                dma((n_dev,)),
            ],
            compiler_params=pltpu.CompilerParams(
                collective_id=0, has_side_effects=True, vmem_limit_bytes=48 * 1024 * 1024),
            cost_estimate=pl.CostEstimate(
                flops=2 * batch * vocab * n_feat, bytes_accessed=2 * vocab * n_feat, transcendentals=2 * batch * vocab),
            name="stream",
        )(hidden_blk.T, scale_blk, cand_ids.T, table_blk)
        log_probs, lse, cand = pl.pallas_call(
            finish_kernel,
            out_shape=[
                jax.ShapeDtypeStruct((batch, vocab), jnp.bfloat16),
                jax.ShapeDtypeStruct((1, batch), jnp.float32),
                jax.ShapeDtypeStruct((n_cand, batch), jnp.float32),
            ],
            in_specs=[vmem_spec, vmem_spec, vmem_spec],
            out_specs=[any_spec, any_spec, any_spec],
            scratch_shapes=[
                pltpu.VMEM((batch, vocab), jnp.bfloat16),
                dma((2 + len(pieces_of(vocab)),)),
            ],
            compiler_params=pltpu.CompilerParams(vmem_limit_bytes=24 * 1024 * 1024),
            name="finish",
        )(capped, lse, cand)
        return lse.reshape(batch), cand.T, log_probs

    return jax.shard_map(
        device_step,
        mesh=mesh,
        in_specs=(P("dp", "tp"), P("dp", None), P("tp"), P("tp", None)),
        out_specs=(P("dp"), P("dp", None), P("dp", "tp")),
        check_vma=False,
    )
```
